256 devices in a mesh: clip: 16 (over z, core), ha: 4 (over x), wa: 4 (over y).
Axes of the slice: x: 4, y: 4, z: 8, core: 2. Of those that a mesh axis runs over, the one named last changes fastest.
Arguments:
- frames: bfloat16 [64, 96, 128, 128], P('clip', 'ha', 'wa'), parts along dimension 0, may hold values from -60 to 60, as said below
- caches: bfloat16 [32, 4, 96, 128, 128], P('clip', None, 'ha', 'wa'), parts along dimension 0, may hold values from -4 to 4
- conv_weights: bfloat16 [4, 3, 3, 3, 128, 128], replicated, may hold values from -0.109375 to 0.109375
- conv_bias: float32 [4, 128], replicated, may hold values from -3 to 3
- norm_gain: float32 [4, 128], replicated, may hold values from 0.25 to 1.75
- norm_shift: float32 [4, 128], replicated, may hold values from -3 to 3
Outputs:
- encoded: bfloat16 [64, 96, 128, 128], P('clip', 'ha', 'wa'), parts along dimension 0
- new_caches: bfloat16 [32, 4, 96, 128, 128], P('clip', None, 'ha', 'wa'), parts along dimension 0
The draws below stay inside these ranges and needn't reach their ends.
There are 16 independent parts, one for each index of `clip`. The reference program is written for one: setup_inputs(seed, part) draws one part's arguments, and reference() takes and returns one part's arrays. A program takes and returns all parts, laid end to end along the dimension named above; an argument that names none is the same for every part. Nothing has to cross between parts.
Inputs may be any that keep to these rules, and one draw needn't show every extreme that they name: `frames`: real-valued features.
All inputs are finite; a program needn't handle non-finite values.
Results may differ from the reference program's by a relative error of at most 0.005.
Values may be sent and summed in bfloat16 or wider, within the bound.
No kernel may reach another device: no remote copies, remote signals or barrier semaphores. Data moves between devices by JAX's collectives and lax.ppermute only.
A program may use at most 64 MiB of HBM per device.

```python
import jax
import jax.numpy as jnp
from jax import lax

C = 128
GROUPS = 32
FR = 4
BLOCKS = 2
CACHE = 2
CONVS = 4
H = 96
W = 128


def draw_frames(key, part):
    streams = jax.random.split(jax.random.fold_in(key, 11), 3)
    row_pos = jnp.arange(H, dtype=jnp.float32) / (H - 1)
    col_pos = jnp.arange(W, dtype=jnp.float32) / (W - 1)
    trend = jnp.log(0.5) + jnp.log(3.0) * 0.5 * (row_pos[:, None] + col_pos[None, :])
    cell_level = jax.random.uniform(streams[0], (FR, H, W, 1), jnp.float32, -1.15, 1.15)
    channel_level = jnp.exp(jax.random.uniform(streams[1], (C,), jnp.float32, -1.15, 1.15))
    noise = jnp.clip(jax.random.normal(streams[2], (FR, H, W, C), jnp.float32), -3.0, 3.0)
    values = jnp.exp(trend[None, :, :, None] + cell_level) * channel_level * noise
    return values.astype(jnp.bfloat16)


def block_scale(stream_key, dims, pieces, low, high):
    factor_of = 1.0
    for dim, shards_of in pieces:
        heights = jax.random.uniform(jax.random.fold_in(jax.random.fold_in(stream_key, 6), dim), (shards_of,), jnp.float32, low / len(pieces), high / len(pieces))
        factor_of = factor_of * jnp.repeat(jnp.exp(heights), dims[dim] // shards_of).reshape((-1,) + (1,) * (len(dims) - 1 - dim))
    return factor_of


def gaussian(key, shape, spread, most, cuts=(), held_as=jnp.bfloat16):
    values = spread * jax.random.normal(key, shape, jnp.float32)
    if cuts:
        values = values * block_scale(key, shape, cuts, -0.22, 0.18)
    return jnp.clip(values, -most, most).astype(held_as)


def setup_inputs(seed: int = 0, part: int = 0) -> dict:
    keys = jax.random.split(jax.random.key(seed), 7)
    part_keys = jax.random.split(jax.random.fold_in(keys[6], part), 7)
    frames = draw_frames(jax.random.fold_in(jax.random.fold_in(keys[6], part), 71), part)
    caches = gaussian(part_keys[1], (CACHE, CONVS, H, W, C), 1.0, 4.0, ((2, 4), (3, 4)))
    conv_weights = gaussian(keys[2], (CONVS, 3, 3, 3, C, C), (27 * C) ** -0.5, 0.109375)
    conv_bias = gaussian(keys[3], (CONVS, C), 0.5, 3.0, (), jnp.float32)
    norm_gain = jnp.clip(1.0 + 0.15 * jax.random.normal(keys[4], (CONVS, C), jnp.float32), 0.25, 1.75)
    norm_shift = gaussian(keys[5], (CONVS, C), 0.5, 3.0, (), jnp.float32)
    return {"frames": frames, "caches": caches, "conv_weights": conv_weights, "conv_bias": conv_bias, "norm_gain": norm_gain, "norm_shift": norm_shift}


EPSILON = 1e-06

def group_norm(values, gain_row, shift_row):
    grouped = values.reshape(values.shape[0], values.shape[1], values.shape[2], GROUPS, -1)
    group_mean = lax.optimization_barrier(jnp.mean(grouped, axis=(0, 1, 2, 4), keepdims=True))
    centered = grouped - group_mean
    variance = lax.optimization_barrier(jnp.mean(centered * centered, axis=(0, 1, 2, 4), keepdims=True))
    normed = centered / jnp.sqrt(variance + EPSILON)
    return normed.reshape(values.shape) * gain_row + shift_row

def causal_conv(activation, history, kernel, bias_row):
    joined = jnp.concatenate([history, activation], axis=0).astype(jnp.float32)
    padded = jnp.pad(joined, ((0, 0), (1, 1), (1, 1), (0, 0)))
    result = lax.conv_general_dilated(padded[None], kernel.astype(jnp.float32), (1, 1, 1), 'VALID', dimension_numbers=('NDHWC', 'DHWIO', 'NDHWC'), precision=lax.Precision.HIGHEST)
    return result[0] + bias_row

def reference(frames, caches, conv_weights, conv_bias, norm_gain, norm_shift):
    block_input = frames
    saved = []
    for block_index in range(BLOCKS):
        first_conv = 2 * block_index
        second_conv = first_conv + 1
        first_act = jax.nn.silu(group_norm(block_input.astype(jnp.float32), norm_gain[first_conv], norm_shift[first_conv])).astype(jnp.bfloat16)
        saved.append(first_act[FR - CACHE:])
        middle = causal_conv(first_act, caches[:, first_conv], conv_weights[first_conv], conv_bias[first_conv])
        second_act = jax.nn.silu(group_norm(middle, norm_gain[second_conv], norm_shift[second_conv])).astype(jnp.bfloat16)
        saved.append(second_act[FR - CACHE:])
        branch = causal_conv(second_act, caches[:, second_conv], conv_weights[second_conv], conv_bias[second_conv])
        block_input = (block_input.astype(jnp.float32) + branch).astype(jnp.bfloat16)
    return (block_input, jnp.stack(saved, axis=1))
```

```python
import functools

import jax
import jax.numpy as jnp
from jax import lax
from jax.experimental import pallas as pl
from jax.experimental.pallas import tpu as pltpu
from jax.sharding import PartitionSpec as P

GROUPS = 32
EPSILON = 1e-06
F32 = jnp.float32
BF16 = jnp.bfloat16
DEPTH = 4
PITCH = 48


def vmem():
    return pl.BlockSpec(memory_space=pltpu.VMEM)


def any_space():
    return pl.BlockSpec(memory_space=pl.ANY)


def in_hbm():
    return pl.BlockSpec(memory_space=pltpu.HBM)


def params(mib):
    return pltpu.CompilerParams(vmem_limit_bytes=mib * 1024 * 1024)


def shifted(arr, axis, step):
    count = lax.axis_size(axis)
    pairs = [(i, i + step) for i in range(count) if 0 <= i + step < count]
    return lax.ppermute(arr, axis, pairs)


def padded(n):
    return -(-n // 16) * 16


class Halo:
    def __init__(self, frames, kept, convs, rows):
        self.fields = [(frames, DEPTH)] + [(kept, DEPTH - k) for k in range(convs)]
        self.rows = rows
        self.line_at, self.cell_at = [0], [0]
        for n, width in self.fields:
            self.line_at.append(self.line_at[-1] + n * width)
            self.cell_at.append(self.cell_at[-1] + padded(n * (rows + 2 * width) * width))


def rows_kernel(frames_ref, caches_ref, head_ref, tail_ref, sems, *, halo):
    rows = halo.rows
    copies = []
    for f, (n, width) in enumerate(halo.fields):
        for t in range(n):
            field = frames_ref.at[t] if f == 0 else caches_ref.at[t, f - 1]
            at = halo.line_at[f] + t * width
            for start, out in ((0, head_ref), (rows - width, tail_ref)):
                copies.append(
                    pltpu.make_async_copy(
                        field.at[pl.ds(start, width)],
                        out.at[pl.ds(at, width)],
                        sems.at[len(copies)],
                    )
                )
    for c in copies:
        c.start()
    for c in copies:
        c.wait()


def sums_kernel(frames_ref, out_ref, *, lines):
    def add(i, carry):
        total, squares = carry
        for u in range(4):
            x = frames_ref[i * 4 + u].astype(F32).reshape(-1, 8, 128)
            total = total + jnp.sum(x, axis=0)
            squares = squares + jnp.sum(x * x, axis=0)
        return total, squares

    zero = jnp.zeros((8, 128), F32)
    total, squares = lax.fori_loop(0, lines // 4, add, (zero, zero))
    spread(out_ref, total, squares)


def spread(out_ref, total, squares):
    out_ref[0:1] = jnp.sum(total, axis=0, keepdims=True)
    out_ref[1:2] = jnp.sum(squares, axis=0, keepdims=True)


def each_line(field, width, rows, north_ref, south_ref, at, frame, use):
    def body(ref, base, shift):
        def step(i, carry):
            use(i + shift, ref[base + i].astype(F32))
            return carry

        return step

    lax.fori_loop(0, width, body(north_ref, at + frame * width, 0), 0)
    lax.fori_loop(0, rows, body(field, 0, width), 0, unroll=2)
    lax.fori_loop(0, width, body(south_ref, at + frame * width, width + rows), 0)


def cols_kernel(frames_ref, caches_ref, north_ref, south_ref, head_ref, tail_ref, a, b, *, halo):
    rows = halo.rows
    cols = frames_ref.shape[2]
    for f, (n, width) in enumerate(halo.fields):
        lines = rows + 2 * width
        for t in range(n):
            field = frames_ref.at[t] if f == 0 else caches_ref.at[t, f - 1]
            base = halo.cell_at[f] + t * lines * width

            def use(r, line, base=base, width=width):
                a[pl.ds(base + r * width, width), :] = line[0:width]
                b[pl.ds(base + r * width, width), :] = line[cols - width : cols]

            each_line(field, width, rows, north_ref, south_ref, halo.line_at[f], t, use)
    head_ref[...] = a[...].astype(BF16)
    tail_ref[...] = b[...].astype(BF16)


def assembled(field, frame, f, halo, north_ref, south_ref, west, east, slot, use):
    _, width = halo.fields[f]
    lines = halo.rows + 2 * width

    def place(r, line):
        cols = line.shape[0]
        at = (frame * lines + r) * width
        slot[pl.ds(width, cols), :] = line
        slot[pl.ds(0, width), :] = west[pl.ds(at, width), :]
        slot[pl.ds(width + cols, width), :] = east[pl.ds(at, width), :]
        use(r)

    each_line(field, width, halo.rows, north_ref, south_ref, halo.line_at[f], frame, place)


def widen(f, halo, west_ref, east_ref, west, east):
    at, end = halo.cell_at[f], halo.cell_at[f + 1]
    west[...] = west_ref[at:end].astype(F32)
    east[...] = east_ref[at:end].astype(F32)


def field_kernel(
    frames_ref, north_ref, south_ref, west_ref, east_ref, out_ref, res_ref, slot, west, east, *, halo
):
    widen(0, halo, west_ref, east_ref, west, east)
    n, width = halo.fields[0]
    lines = halo.rows + 2 * width
    pitch = out_ref.shape[1]
    for t in range(n):

        def use(r, t=t):
            out_ref[t * lines + r] = slot[0:pitch, :].astype(BF16)

            @pl.when((r >= 2) & (r < lines - 2))
            def _():
                res_ref[t, r - 2] = slot[pl.ds(2, pitch), :].astype(BF16)

        assembled(frames_ref.at[t], t, 0, halo, north_ref, south_ref, west, east, slot, use)


def group_total(rows):
    lanes = lax.broadcasted_iota(jnp.int32, rows.shape, 1)
    c = rows.shape[-1]
    per = c // GROUPS
    step = 1
    while step < per:
        up = pltpu.roll(rows, c - step, 1)
        down = pltpu.roll(rows, step, 1)
        rows = rows + jnp.where((lanes // step) % 2 == 0, up, down)
        step *= 2
    return rows


def taps_into(buf, slot_ref, index, pitch):
    for dw in range(3):
        buf[index, :, dw * 128 : (dw + 1) * 128] = slot_ref[pl.ds(dw, pitch), :].astype(BF16)


def lhs_of(buf, frame, lines_in, start, lines, pitch):
    parts = [
        buf[pl.ds(frame * lines_in + start + dh, lines)].reshape(lines * pitch, 384)
        for dh in range(3)
    ]
    return jnp.concatenate(parts, axis=1)


def kept_kernel(*refs, k, halo, pitch, chunk, shift):
    refs = list(refs)
    caches_ref, north_ref, south_ref, west_ref, east_ref, w_ref, bias_ref = refs[:7]
    refs = refs[7:]
    v_ref = refs.pop(0) if shift else None
    out_ref = refs.pop(0)
    res_ref = refs.pop(0) if shift else None
    slot, west, east, buf = refs
    f = k + 1
    widen(f, halo, west_ref, east_ref, west, east)
    n, width = halo.fields[f]
    lines_in = halo.rows + 2 * width
    lines_out = lines_in - 2
    for t in range(n):
        assembled(
            caches_ref.at[t, k],
            t,
            f,
            halo,
            north_ref,
            south_ref,
            west,
            east,
            slot,
            lambda r, t=t: taps_into(buf, slot, t * lines_in + r, pitch),
        )
    zero = jnp.zeros((1152, 128), BF16)

    def conv(c, carry):
        start = c * chunk
        left = [lhs_of(buf, t, lines_in, start, chunk, pitch) for t in range(2)]
        w = jnp.concatenate(
            [
                jnp.concatenate([w_ref[k, 0], w_ref[k, 1]], axis=0),
                jnp.concatenate([zero, w_ref[k, 0]], axis=0),
            ],
            axis=1,
        )
        acc = jnp.dot(jnp.concatenate(left, axis=1), w, preferred_element_type=F32)
        for t in range(2):
            part = acc[:, t * 128 : (t + 1) * 128] + bias_ref[k : k + 1]
            out_ref[t, pl.ds(start, chunk)] = part.reshape(chunk, pitch, 128)
        return carry

    lax.fori_loop(0, lines_out // chunk, conv, 0)
    if shift:
        frames, rows, cols, _ = res_ref.shape
        for t in range(frames):

            def move(r, carry, t=t):
                slot[0:48, :] = v_ref[t, r + 2].astype(F32)
                res_ref[t, r] = slot[pl.ds(2, cols), :].astype(BF16)
                return carry

            lax.fori_loop(0, rows, move, 0, unroll=2)


def main_kernel(
    *refs, k, lines_in, width, halo, pitch, chunk, rows, cols, cells, residual, last
):
    refs = list(refs)
    v_ref, sums_ref, gain_ref, shift_ref, bias_ref, kept_ref, w_ref = refs[:7]
    refs = refs[7:]
    res_ref = refs.pop(0) if residual else None
    if last:
        earlier = refs[:3]
        final_ref, caches_ref, slots, buf, out_ref, saved_ref, sems = refs[3:]
    else:
        out_ref, stats_ref, saved_ref, slots, buf = refs
    lines_out = lines_in - 2
    ha, wa = lax.axis_index("ha"), lax.axis_index("wa")
    last_h, last_w = lax.axis_size("ha") - 1, lax.axis_size("wa") - 1
    row_lo = jnp.where(ha == 0, halo, 0)
    row_hi = jnp.where(ha == last_h, halo + rows, lines_in)
    col_lo = jnp.where(wa == 0, halo, 0)
    col_hi = jnp.where(wa == last_w, halo + cols, width)
    copies = []
    if last:
        for j, ref in enumerate(earlier):
            copies.append(pltpu.make_async_copy(ref, caches_ref.at[:, j], sems.at[j]))
        for c in copies:
            c.start()

    totals = group_total(sums_ref[...])
    mean = totals[0:1] / cells
    variance = totals[1:2] / cells - mean * mean
    scale = lax.rsqrt(variance + EPSILON)
    mult = 0.5 * scale * gain_ref[k : k + 1]
    offset = 0.5 * shift_ref[k : k + 1] - mean * mult
    held = v_ref.shape[1]
    at_col = lax.broadcasted_iota(jnp.int32, (held, 128), 0)

    def act(base, unroll, save):
        def step(i, carry):
            for u in range(unroll):
                at = base + i * unroll + u
                r = lax.rem(at, lines_in)
                slot = slots.at[u]
                z = v_ref[at].astype(F32) * mult + offset
                a = z + z * jnp.tanh(z)
                hi = jnp.where((r >= row_lo) & (r < row_hi), col_hi, 0)
                slot[0:held, :] = jnp.where((at_col >= col_lo) & (at_col < hi), a, 0.0)
                taps_into(buf, slot, at, pitch)
                if save is not None:
                    saved_ref[save, r - halo] = slot[pl.ds(halo, cols), :].astype(BF16)
            return carry

        return step

    lax.fori_loop(0, 2 * lines_in // 4, act(0, 4, None), 0)
    for t in (2, 3):
        base = t * lines_in
        lax.fori_loop(0, halo, act(base, 1, None), 0)
        lax.fori_loop(0, rows // 4, act(base + halo, 4, t - 2), 0)
        lax.fori_loop(0, halo, act(base + halo + rows, 1, None), 0)
    if last:
        copies.append(pltpu.make_async_copy(saved_ref, caches_ref.at[:, 3], sems.at[3]))
        copies[3].start()

    zero = jnp.zeros((1152, 128), BF16)
    inner = halo - 1
    line = lax.broadcasted_iota(jnp.int32, (chunk, pitch, 128), 0)
    col = lax.broadcasted_iota(jnp.int32, (chunk, pitch, 128), 1)

    def finish(t, start, part, carry):
        part = part.reshape(chunk, pitch, 128)
        if t < 2:
            part = part + kept_ref[t, pl.ds(start, chunk)]
        else:
            part = part + bias_ref[k : k + 1][None]
        if residual:
            part = part + res_ref[t, pl.ds(start, chunk)].astype(F32)
        out = part.astype(out_ref.dtype)
        out_ref[t, pl.ds(start, chunk)] = out
        if last:
            return carry
        part = out.astype(F32)
        at = line + start
        keep = (at >= inner) & (at < inner + rows) & (col >= inner) & (col < inner + cols)
        part = jnp.where(keep, part, 0.0)
        total, squares = carry
        total = total + jnp.sum(part.reshape(-1, 8, 128), axis=0)
        squares = squares + jnp.sum((part * part).reshape(-1, 8, 128), axis=0)
        return total, squares

    def conv(c, carry):
        start = c * chunk
        left = [lhs_of(buf, t, lines_in, start, chunk, pitch) for t in range(4)]
        w01 = jnp.concatenate(
            [
                jnp.concatenate([w_ref[k, 2], zero], axis=0),
                jnp.concatenate([w_ref[k, 1], w_ref[k, 2]], axis=0),
            ],
            axis=1,
        )
        acc = jnp.dot(jnp.concatenate(left[:2], axis=1), w01, preferred_element_type=F32)
        carry = finish(0, start, acc[:, :128], carry)
        carry = finish(1, start, acc[:, 128:], carry)
        w23 = jnp.concatenate(
            [
                jnp.concatenate([w_ref[k, 0], w_ref[k, 1], w_ref[k, 2], zero], axis=0),
                jnp.concatenate([zero, w_ref[k, 0], w_ref[k, 1], w_ref[k, 2]], axis=0),
            ],
            axis=1,
        )
        acc = jnp.dot(jnp.concatenate(left, axis=1), w23, preferred_element_type=F32)
        carry = finish(2, start, acc[:, :128], carry)
        carry = finish(3, start, acc[:, 128:], carry)
        return carry

    none = jnp.zeros((8, 128), F32)
    total, squares = lax.fori_loop(0, lines_out // chunk, conv, (none, none))
    if last:
        copies.append(pltpu.make_async_copy(out_ref, final_ref, sems.at[4]))
        copies[4].start()
        for c in copies:
            c.wait()
    else:
        spread(stats_ref, total, squares)


def kept_part(k, halo, caches, north, south, west, east, w, bias, pitch, chunk, v=None):
    n, width = halo.fields[k + 1]
    lines_in = halo.rows + 2 * width
    cells = halo.cell_at[k + 2] - halo.cell_at[k + 1]
    args = [caches, north, south, west, east, w, bias]
    outs = [jax.ShapeDtypeStruct((2, lines_in - 2, pitch, 128), F32)]
    if v is not None:
        args.append(v)
        outs.append(
            jax.ShapeDtypeStruct((v.shape[0], halo.rows, caches.shape[3], 128), BF16)
        )
    done = pl.pallas_call(
        functools.partial(
            kept_kernel, k=k, halo=halo, pitch=pitch, chunk=chunk, shift=v is not None
        ),
        out_shape=tuple(outs),
        in_specs=[vmem()] * len(args),
        out_specs=(vmem(),) * len(outs),
        scratch_shapes=[
            pltpu.VMEM((56, 128), F32),
            pltpu.VMEM((cells, 128), F32),
            pltpu.VMEM((cells, 128), F32),
            pltpu.VMEM((n * lines_in, pitch, 384), BF16),
        ],
        cost_estimate=pl.CostEstimate(
            flops=2 * lines_in * pitch * 2304 * 256, bytes_accessed=4000000, transcendentals=0
        ),
        compiler_params=params(8),
        name="kept",
    )(*args)
    return done if v is not None else (done[0], None)


def main_part(k, v, sums, gain, shift, bias, kept, w, res, earlier, halo, width, rows, cols, chunk, cells, dtype):
    held = v.shape[-2]
    _, lines_out, pitch, _ = kept.shape
    lines_in = lines_out + 2
    v = v.reshape(-1, held, 128)
    frames = v.shape[0] // lines_in
    last = earlier is not None
    args = [v, sums, gain, shift, bias, kept, w]
    if res is not None:
        args.append(res)
    out = (frames, lines_out, pitch, 128)
    saved = (2, rows, cols, 128)
    scratch = [
        pltpu.VMEM((4, 56, 128), F32),
        pltpu.VMEM((frames * lines_in, pitch, 384), BF16),
    ]
    if last:
        args += earlier
        outs = (
            jax.ShapeDtypeStruct(out, dtype),
            jax.ShapeDtypeStruct((2, 1 + len(earlier), rows, cols, 128), BF16),
        )
        out_specs = (any_space(), any_space())
        scratch += [
            pltpu.VMEM(out, dtype),
            pltpu.VMEM(saved, BF16),
            pltpu.SemaphoreType.DMA((5,)),
        ]
    else:
        outs = (
            jax.ShapeDtypeStruct(out, dtype),
            jax.ShapeDtypeStruct(sums.shape, F32),
            jax.ShapeDtypeStruct(saved, BF16),
        )
        out_specs = (vmem(),) * 3
    return pl.pallas_call(
        functools.partial(
            main_kernel,
            k=k,
            lines_in=lines_in,
            width=width,
            halo=halo,
            pitch=pitch,
            chunk=chunk,
            rows=rows,
            cols=cols,
            cells=cells,
            residual=res is not None,
            last=last,
        ),
        out_shape=outs,
        in_specs=[vmem()] * len(args),
        out_specs=out_specs,
        scratch_shapes=scratch,
        cost_estimate=pl.CostEstimate(
            flops=2 * lines_in * pitch * 6912 * 256, bytes_accessed=10000000, transcendentals=0
        ),
        compiler_params=params(14),
        name="conv",
    )(*args)


def over_axis(sums, axis):
    count = lax.axis_size(axis)
    return sums + sum(
        lax.ppermute(sums, axis, [(i, i ^ step) for i in range(count)]) for step in range(1, count)
    )


def everyone(sums):
    return over_axis(over_axis(sums, "ha"), "wa")


def local(frames, caches, conv_weights, conv_bias, norm_gain, norm_shift):
    n, rows, cols, c = frames.shape
    peers = lax.axis_size(("ha", "wa"))
    cells = float(n * rows * cols * peers * (c // GROUPS))
    kept_n, convs = caches.shape[:2]
    weights = conv_weights.reshape(convs, 3, 9 * c, c)
    halo = Halo(n, kept_n, convs, rows)

    lines = jax.ShapeDtypeStruct((halo.line_at[-1], cols, c), BF16)
    count = 2 * (n + kept_n * convs)
    head, tail = pl.pallas_call(
        functools.partial(rows_kernel, halo=halo),
        out_shape=(lines, lines),
        in_specs=[in_hbm()] * 2,
        out_specs=(vmem(), vmem()),
        scratch_shapes=[pltpu.SemaphoreType.DMA((count,))],
        compiler_params=params(4),
        name="rows",
    )(frames, caches)
    north, south = shifted(tail, "ha", 1), shifted(head, "ha", -1)
    sums = pl.pallas_call(
        functools.partial(sums_kernel, lines=n * rows),
        out_shape=jax.ShapeDtypeStruct((2, c), F32),
        in_specs=[vmem()],
        out_specs=vmem(),
        compiler_params=params(4),
        name="sums",
    )(frames.reshape(n * rows, cols, c))
    sums = everyone(sums)
    strip = jax.ShapeDtypeStruct((halo.cell_at[-1], c), BF16)
    head, tail = pl.pallas_call(
        functools.partial(cols_kernel, halo=halo),
        out_shape=(strip, strip),
        in_specs=[vmem()] * 4,
        out_specs=(vmem(), vmem()),
        scratch_shapes=[pltpu.VMEM(strip.shape, F32)] * 2,
        compiler_params=params(4),
        name="cols",
    )(frames, caches, north, south)
    west, east = shifted(tail, "wa", 1), shifted(head, "wa", -1)
    around = (north, south, west, east)

    wide = rows + 2 * DEPTH
    side = pltpu.VMEM((halo.cell_at[1], c), F32)
    v, res = pl.pallas_call(
        functools.partial(field_kernel, halo=halo),
        out_shape=(
            jax.ShapeDtypeStruct((n * wide, PITCH, c), BF16),
            jax.ShapeDtypeStruct((n, wide - 4, PITCH, c), BF16),
        ),
        in_specs=[vmem()] * 5,
        out_specs=(vmem(), vmem()),
        scratch_shapes=[pltpu.VMEM((56, c), F32), side, side],
        compiler_params=params(4),
        name="field",
    )(frames, *around)

    chunks = (10, 7, 13, 12)
    pitches = (PITCH, PITCH, PITCH, cols)
    saved = []
    width = cols + 2 * DEPTH
    for k in range(convs):
        last = k == convs - 1
        kept, moved = kept_part(
            k,
            halo,
            caches,
            *around,
            weights,
            conv_bias,
            pitches[k],
            chunks[k],
            v=block if last else None,
        )
        if last:
            res = moved
        done = main_part(
            k,
            v,
            sums,
            norm_gain,
            norm_shift,
            conv_bias,
            kept,
            weights,
            res if k % 2 else None,
            saved if last else None,
            DEPTH - k,
            width,
            rows,
            cols,
            chunks[k],
            cells,
            BF16 if k % 2 else F32,
        )
        if last:
            return done
        v, sums, keep = done
        if k % 2:
            block = v
        width -= 2
        saved.append(keep)
        sums = everyone(sums)


def solution(mesh):
    return jax.shard_map(
        local,
        mesh=mesh,
        in_specs=(
            P("clip", "ha", "wa", None),
            P("clip", None, "ha", "wa", None),
            P(),
            P(),
            P(),
            P(),
        ),
        out_specs=(P("clip", "ha", "wa", None), P("clip", None, "ha", "wa", None)),
        check_vma=False,
    )
```

```python
import functools

import jax
import jax.numpy as jnp
from jax import lax
from jax.experimental import pallas as pl
from jax.experimental.pallas import tpu as pltpu
from jax.sharding import PartitionSpec as P

GROUPS = 32
EPSILON = 1e-06
F32 = jnp.float32
BF16 = jnp.bfloat16
LINES = 32
ROWS_MIB = 58
PITCH = 48
LEAD = 8


def vmem():
    return pl.BlockSpec(memory_space=pltpu.VMEM)


def any_space():
    return pl.BlockSpec(memory_space=pl.ANY)


def in_hbm():
    return pl.BlockSpec(memory_space=pltpu.HBM)


def params(mib):
    return pltpu.CompilerParams(vmem_limit_bytes=mib * 1024 * 1024)


def around(arr, axis, step):
    count = lax.axis_size(axis)
    return lax.ppermute(arr, axis, [(i, (i + step) % count) for i in range(count)])


class Halo:
    def __init__(self, rows, fields):
        self.rows, self.fields = rows, fields
        self.at = [0]
        for n, width in fields:
            self.at.append(self.at[-1] + n * width)
        self.sums = self.at[-1]
        self.count = self.sums + 1


def encoded(sums):
    rows = []
    for i in range(2):
        rest = sums[i : i + 1]
        for _ in range(3):
            part = rest.astype(BF16).astype(F32)
            rows.append(part)
            rest = rest - part
    rows.append(jnp.zeros((LINES - 6, 128), F32))
    return jnp.concatenate(rows, axis=0).astype(BF16)


def decoded(block):
    x = block[0:8].astype(F32)
    return jnp.concatenate(
        [x[0:1] + x[1:2] + x[2:3], x[3:4] + x[4:5] + x[5:6]], axis=0
    )


def two_rows(total, squares):
    return jnp.concatenate(
        [jnp.sum(total, axis=0, keepdims=True), jnp.sum(squares, axis=0, keepdims=True)], axis=0
    )


def rows_kernel(frames_ref, caches_ref, head_ref, tail_ref, sums_ref, held, sems, *, halo):
    rows = halo.rows
    copies = []
    n = held.shape[0]
    for t in range(n):
        copies.append(pltpu.make_async_copy(frames_ref.at[t], held.at[t], sems.at[t]))
    for f, (m, width) in enumerate(halo.fields):
        for t in range(m):
            field = frames_ref.at[t] if f == 0 else caches_ref.at[t, f - 1]
            at = halo.at[f] + t * width
            for start, out in ((0, head_ref), (rows - width, tail_ref)):
                copies.append(
                    pltpu.make_async_copy(
                        field.at[pl.ds(start, width)],
                        out.at[pl.ds(at, width)],
                        sems.at[len(copies)],
                    )
                )
    for c in copies:
        c.start()
    total = squares = jnp.zeros((8, 128), F32)
    for t in range(n):
        copies[t].wait()

        def add(i, carry, t=t):
            total, squares = carry
            for u in range(4):
                x = held[t, 4 * i + u].astype(F32).reshape(-1, 8, 128)
                total = total + jnp.sum(x, axis=0)
                squares = squares + jnp.sum(x * x, axis=0)
            return total, squares

        total, squares = lax.fori_loop(0, rows // 4, add, (total, squares))
    sums = two_rows(total, squares)
    sums_ref[...] = sums
    code = encoded(sums)
    head_ref[halo.sums] = code
    tail_ref[halo.sums] = code
    for c in copies[n:]:
        c.wait()


def cols_kernel(*refs, halo):
    refs = list(refs)
    field_ref = refs.pop(0)
    caches_ref = refs.pop(0) if len(halo.fields) > 1 else None
    north_ref, south_ref, far_ref, own_ref, head_ref, tail_ref, sums_ref, flat = refs
    rows = halo.rows
    cols = field_ref.shape[2]
    for f, (n, width) in enumerate(halo.fields):
        for t in range(n):
            field = field_ref.at[t] if f == 0 else caches_ref.at[t, f - 1]
            base = halo.at[f] + t * width

            def put(line, ref, i):
                x = jnp.concatenate([ref[i, 0:8], ref[i, cols - 8 : cols]], axis=0)
                flat[pl.ds(pl.multiple_of(line * 16, 8), 16), :] = x.astype(F32)

            for i in range(width):
                put(i, north_ref, base + i)
                put(width + rows + i, south_ref, base + i)

            def step(i, carry, put=put, field=field, width=width):
                for u in range(4):
                    put(width + 4 * i + u, field, 4 * i + u)
                return carry

            lax.fori_loop(0, rows // 4, step, 0)
            for j in range(width):
                head_ref[base + j] = flat[pl.ds(j, LINES, stride=16), :].astype(BF16)
                tail_ref[base + j] = flat[pl.ds(16 - width + j, LINES, stride=16), :].astype(BF16)
    sums = own_ref[...] + far_ref[...]
    sums = sums + decoded(north_ref[halo.sums]) + decoded(south_ref[halo.sums])
    sums_ref[...] = sums
    code = encoded(sums)
    head_ref[halo.sums] = code
    tail_ref[halo.sums] = code


def group_total(rows):
    lanes = lax.broadcasted_iota(jnp.int32, rows.shape, 1)
    c = rows.shape[-1]
    per = c // GROUPS
    step = 1
    while step < per:
        up = pltpu.roll(rows, c - step, 1)
        down = pltpu.roll(rows, step, 1)
        rows = rows + jnp.where((lanes // step) % 2 == 0, up, down)
        step *= 2
    return rows


class Stage:
    def __init__(self, halo, rows, cols, buf, quad, flat, side):
        self.halo, self.rows, self.cols = halo, rows, cols
        self.lines = rows + 2 * halo
        self.strips = 2 * (halo - 1)
        self.buf, self.quad, self.flat, self.side = buf, quad, flat, side

    def put(self, t, line, a):
        b = a.astype(BF16)
        self.flat[pl.ds(pl.multiple_of(line * PITCH + LEAD, 8), self.cols), :] = a
        self.buf[t * self.lines + line, :, 128:256] = b
        return b

    def put_strip(self, j, a):
        self.side[j, 0:LINES] = a

    def close(self, t):
        h, cols, flat, side = self.halo, self.cols, self.flat, self.side
        flat[pl.ds(LEAD - 1, LINES, stride=PITCH), :] = side[h - 1, 0:LINES]
        flat[pl.ds(LEAD + cols, LINES, stride=PITCH), :] = side[h, 0:LINES]
        if self.strips:
            side[2 * h, 0:LINES] = flat[pl.ds(LEAD, LINES, stride=PITCH), :]
            side[2 * h + 1, 0:LINES] = flat[pl.ds(LEAD + cols - 1, LINES, stride=PITCH), :]
            order = list(range(h)) + [2 * h, 2 * h + 1] + list(range(h, 2 * h))
            for q, j in enumerate(order):
                for dh in range(3):
                    self.quad[t * (2 * h + 2) + q, :, dh * 128 : (dh + 1) * 128] = side[
                        j, pl.ds(dh, LINES)
                    ].astype(BF16)

        def step(i, carry):
            for u in range(2):
                line = 2 * i + u
                for dw in (0, 2):
                    at = line * PITCH + LEAD - 1 + dw
                    self.buf[t * self.lines + line, :, dw * 128 : (dw + 1) * 128] = flat[
                        pl.ds(at, cols), :
                    ].astype(BF16)
            return carry

        lax.fori_loop(0, self.lines // 2, step, 0)

    def lhs(self, t, c, chunk, strips):
        h = self.halo
        parts = [
            self.buf[pl.ds(t * self.lines + c * chunk + dh, chunk)].reshape(chunk * self.cols, 384)
            for dh in range(3)
        ]
        blocks = [jnp.concatenate(parts, axis=1)]
        for u in range(strips):
            strip = c * strips + u
            q = t * (2 * h + 2) + strip + jnp.where(strip >= h - 1, 2, 0)
            blocks.append(
                jnp.concatenate(
                    [
                        self.quad[q + dw, :, dh * 128 : (dh + 1) * 128]
                        for dh in range(3)
                        for dw in range(3)
                    ],
                    axis=1,
                )
            )
        return jnp.concatenate(blocks, axis=0)


def edges():
    ha, wa = lax.axis_index("ha"), lax.axis_index("wa")
    return ha > 0, ha < lax.axis_size("ha") - 1, wa > 0, wa < lax.axis_size("wa") - 1


def kept_kernel(*refs, k, halo, cols, chunk, strips):
    caches_ref, north_ref, south_ref, west_ref, east_ref, w_ref, bias_ref, out_ref = refs[:8]
    strip_ref = refs[8] if strips else None
    buf, quad, flat, side = refs[-4:]
    rows = halo.rows
    n, h = halo.fields[k + 1]
    stage = Stage(h, rows, cols, buf, quad, flat, side)
    up, down, left, right = edges()
    lines = stage.lines
    at_line = lax.broadcasted_iota(jnp.int32, (LINES, 128), 0)
    inside = (at_line >= jnp.where(up, 0, h)) & (at_line < jnp.where(down, lines, h + rows))
    for t in range(n):
        base = halo.at[k + 1] + t * h
        for i in range(h):
            stage.put(t, i, jnp.where(up, north_ref[base + i].astype(F32), 0.0))
            stage.put(t, h + rows + i, jnp.where(down, south_ref[base + i].astype(F32), 0.0))
            stage.put_strip(i, jnp.where(inside & left, west_ref[base + i].astype(F32), 0.0))
            stage.put_strip(h + i, jnp.where(inside & right, east_ref[base + i].astype(F32), 0.0))

        def step(i, carry, t=t):
            for u in range(4):
                stage.put(t, h + 4 * i + u, caches_ref[t, k, 4 * i + u].astype(F32))
            return carry

        lax.fori_loop(0, rows // 4, step, 0)
        stage.close(t)
    zero = jnp.zeros((1152, 128), BF16)

    def conv(c, carry):
        left = [stage.lhs(t, c, chunk, strips) for t in range(2)]
        w = jnp.concatenate(
            [
                jnp.concatenate([w_ref[k, 0], w_ref[k, 1]], axis=0),
                jnp.concatenate([zero, w_ref[k, 0]], axis=0),
            ],
            axis=1,
        )
        acc = jnp.dot(jnp.concatenate(left, axis=1), w, preferred_element_type=F32)
        for t in range(2):
            part = acc[:, t * 128 : (t + 1) * 128] + bias_ref[k : k + 1]
            cut = chunk * cols
            out_ref[t, pl.ds(c * chunk, chunk)] = part[:cut].reshape(chunk, cols, 128)
            for u in range(strips):
                strip_ref[t, c * strips + u] = part[cut + u * LINES : cut + (u + 1) * LINES]
        return carry

    lax.fori_loop(0, (stage.lines - 2) // chunk, conv, 0)


def main_kernel(*refs, k, halo, cols, chunk, strips, cells, last):
    refs = list(refs)
    rows = halo.rows
    _, h = halo.fields[k + 1]
    odd = k % 2 == 1
    frames = 4
    if odd:
        v_ref, v_strip_ref, sums_ref = refs[:3]
        refs = refs[3:]
        sums = sums_ref[...]
    else:
        v_ref, north_ref, south_ref, west_ref, east_ref, far_ref, own_ref = refs[:7]
        refs = refs[7:]
        at_sums = west_ref.shape[0] - 1
        sums = own_ref[...] + far_ref[...]
        sums = sums + decoded(west_ref[at_sums]) + decoded(east_ref[at_sums])
    gain_ref, shift_ref, bias_ref, w_ref, kept_ref = refs[:5]
    refs = refs[5:]
    kept_strip_ref = None if odd else refs.pop(0)
    res_ref = refs.pop(0) if odd else None
    if last:
        earlier = refs[:3]
        final_ref, caches_ref = refs[3:5]
        buf, quad, flat, side, out_ref, saved_ref, sems = refs[5:]
    elif odd:
        out_ref, head_ref, tail_ref, stats_ref, saved_ref, buf, quad, flat, side = refs
    else:
        out_ref, strip_ref, stats_ref, saved_ref, buf, quad, flat, side = refs
    stage = Stage(h, rows, cols, buf, quad, flat, side)
    lines = stage.lines
    up, down, left, right = edges()
    at_line = lax.broadcasted_iota(jnp.int32, (LINES, 128), 0)
    inside = (at_line >= jnp.where(up, 0, h)) & (at_line < jnp.where(down, lines, h + rows))
    copies = []
    if last:
        for j, ref in enumerate(earlier):
            copies.append(pltpu.make_async_copy(ref, caches_ref.at[:, j], sems.at[j]))
        for c in copies:
            c.start()

    totals = group_total(sums)
    mean = totals[0:1] / cells
    variance = totals[1:2] / cells - mean * mean
    scale = lax.rsqrt(variance + EPSILON)
    mult = 0.5 * scale * gain_ref[k : k + 1]
    offset = 0.5 * shift_ref[k : k + 1] - mean * mult

    def act(x):
        z = x.astype(F32) * mult + offset
        return z + z * jnp.tanh(z)

    for t in range(frames):
        base = t * h
        for i in range(h):
            top = v_ref[t, i] if odd else north_ref[base + i]
            low = v_ref[t, h + rows + i] if odd else south_ref[base + i]
            west = v_strip_ref[t, i] if odd else west_ref[base + i]
            east = v_strip_ref[t, h + i] if odd else east_ref[base + i]
            stage.put(t, i, jnp.where(up, act(top), 0.0))
            stage.put(t, h + rows + i, jnp.where(down, act(low), 0.0))
            stage.put_strip(i, jnp.where(inside & left, act(west), 0.0))
            stage.put_strip(h + i, jnp.where(inside & right, act(east), 0.0))

        def inner(i, carry, t=t):
            for u in range(4):
                r = 4 * i + u
                b = stage.put(t, h + r, act(v_ref[t, h + r if odd else r]))
                if t >= frames - 2:
                    saved_ref[t - frames + 2, r] = b
            return carry

        lax.fori_loop(0, rows // 4, inner, 0)
        stage.close(t)
    if last:
        copies.append(pltpu.make_async_copy(saved_ref, caches_ref.at[:, 3], sems.at[3]))
        copies[3].start()

    zero = jnp.zeros((1152, 128), BF16)
    edge = h - 1
    line = lax.broadcasted_iota(jnp.int32, (chunk, cols, 128), 0)
    cut = chunk * cols

    def finish(t, c, part, carry):
        at = pl.ds(c * chunk, chunk)
        for u in range(strips):
            x = part[cut + u * LINES : cut + (u + 1) * LINES]
            strip = c * strips + u
            x = x + (kept_strip_ref[t, strip] if t < 2 else bias_ref[k : k + 1])
            strip_ref[t, strip] = x.astype(strip_ref.dtype)
        x = part[:cut].reshape(chunk, cols, 128)
        x = x + (kept_ref[t, at] if t < 2 else bias_ref[k : k + 1][None])
        if odd:
            x = x + res_ref[t, at].astype(F32)
        out = x.astype(out_ref.dtype)
        out_ref[t, at] = out
        if last:
            return carry
        x = out.astype(F32)
        if edge:
            where = line + c * chunk
            x = jnp.where((where >= edge) & (where < edge + rows), x, 0.0)
        total, squares = carry
        total = total + jnp.sum(x.reshape(-1, 8, 128), axis=0)
        squares = squares + jnp.sum((x * x).reshape(-1, 8, 128), axis=0)
        return total, squares

    def conv(c, carry):
        left = [stage.lhs(t, c, chunk, strips) for t in range(frames)]
        w01 = jnp.concatenate(
            [
                jnp.concatenate([w_ref[k, 2], zero], axis=0),
                jnp.concatenate([w_ref[k, 1], w_ref[k, 2]], axis=0),
            ],
            axis=1,
        )
        acc = jnp.dot(jnp.concatenate(left[:2], axis=1), w01, preferred_element_type=F32)
        carry = finish(0, c, acc[:, :128], carry)
        carry = finish(1, c, acc[:, 128:], carry)
        w23 = jnp.concatenate(
            [
                jnp.concatenate([w_ref[k, 0], w_ref[k, 1], w_ref[k, 2], zero], axis=0),
                jnp.concatenate([zero, w_ref[k, 0], w_ref[k, 1], w_ref[k, 2]], axis=0),
            ],
            axis=1,
        )
        acc = jnp.dot(jnp.concatenate(left, axis=1), w23, preferred_element_type=F32)
        carry = finish(2, c, acc[:, :128], carry)
        carry = finish(3, c, acc[:, 128:], carry)
        return carry

    none = jnp.zeros((8, 128), F32)
    total, squares = lax.fori_loop(0, (lines - 2) // chunk, conv, (none, none))
    if last:
        copies.append(pltpu.make_async_copy(out_ref, final_ref, sems.at[4]))
        copies[4].start()
        for c in copies:
            c.wait()
        return
    sums = two_rows(total, squares)
    stats_ref[...] = sums
    if odd:
        width = (head_ref.shape[0] - 1) // frames
        for t in range(frames):
            for i in range(width):
                head_ref[t * width + i] = out_ref[t, i]
                tail_ref[t * width + i] = out_ref[t, rows - width + i]
        code = encoded(sums)
        head_ref[frames * width] = code
        tail_ref[frames * width] = code


CHUNKS = ((13, 1), (12, 0), (13, 1), (12, 0))
WIDTHS = (2, 1, 2, 1)


def stage_scratch(halo, k, frames, cols):
    _, h = halo.fields[k + 1]
    lines = halo.rows + 2 * h
    return [
        pltpu.VMEM((frames * lines, cols, 384), BF16),
        pltpu.VMEM((frames * (2 * h + 2), LINES, 384), BF16),
        pltpu.VMEM((LINES * PITCH, 128), F32),
        pltpu.VMEM((2 * h + 2, LINES + 8, 128), F32),
    ]


def flops(halo, k, cols, terms):
    _, h = halo.fields[k + 1]
    cells = (halo.rows + 2 * h - 2) * cols + 2 * (h - 1) * LINES
    return pl.CostEstimate(
        flops=2 * cells * terms * 256, bytes_accessed=4000000, transcendentals=0
    )


def kept_part(k, halo, caches, sides, w, bias):
    n, h = halo.fields[k + 1]
    cols = caches.shape[3]
    chunk, strips = CHUNKS[k]
    args = [caches, *sides, w, bias]
    outs = [jax.ShapeDtypeStruct((n, halo.rows + 2 * h - 2, cols, 128), F32)]
    if strips:
        outs.append(jax.ShapeDtypeStruct((n, 2 * (h - 1), LINES, 128), F32))
    return pl.pallas_call(
        functools.partial(kept_kernel, k=k, halo=halo, cols=cols, chunk=chunk, strips=strips),
        out_shape=tuple(outs),
        in_specs=[vmem()] * len(args),
        out_specs=(vmem(),) * len(outs),
        scratch_shapes=stage_scratch(halo, k, n, cols),
        cost_estimate=flops(halo, k, cols, 2304),
        compiler_params=params(8),
        name="kept",
    )(*args)


def main_part(k, halo, field, gain, shift, bias, w, kept, res, earlier, send, cells):
    frames, cols = field[0].shape[0], field[0].shape[2]
    _, h = halo.fields[k + 1]
    lines_out = halo.rows + 2 * h - 2
    chunk, strips = CHUNKS[k]
    last = earlier is not None
    dtype = BF16 if k % 2 else F32
    args = [*field, gain, shift, bias, w, *kept, *res]
    out = (frames, lines_out, cols, 128)
    saved = (2, halo.rows, cols, 128)
    scratch = stage_scratch(halo, k, frames, cols)
    outs = [jax.ShapeDtypeStruct(out, dtype)]
    if last:
        args += earlier
        outs.append(jax.ShapeDtypeStruct((2, 1 + len(earlier), halo.rows, cols, 128), BF16))
        out_specs = (any_space(), any_space())
        scratch += [
            pltpu.VMEM(out, dtype),
            pltpu.VMEM(saved, BF16),
            pltpu.SemaphoreType.DMA((5,)),
        ]
    else:
        if k % 2:
            outs += [jax.ShapeDtypeStruct((send, cols, 128), BF16)] * 2
        else:
            outs.append(jax.ShapeDtypeStruct((frames, 2 * (h - 1), LINES, 128), dtype))
        outs.append(jax.ShapeDtypeStruct((2, 128), F32))
        outs.append(jax.ShapeDtypeStruct(saved, BF16))
        out_specs = (vmem(),) * len(outs)
    return pl.pallas_call(
        functools.partial(
            main_kernel,
            k=k,
            halo=halo,
            cols=cols,
            chunk=chunk,
            strips=strips,
            cells=cells,
            last=last,
        ),
        out_shape=tuple(outs),
        in_specs=[vmem()] * len(args),
        out_specs=out_specs,
        scratch_shapes=scratch,
        cost_estimate=flops(halo, k, cols, 6912),
        compiler_params=params(14),
        name="conv",
    )(*args)


def cols_part(halo, field, caches, north, south, far, own):
    c = field.shape[-1]
    strips = jax.ShapeDtypeStruct((halo.count, LINES, c), BF16)
    args = [field, *caches, north, south, far, own]
    return pl.pallas_call(
        functools.partial(cols_kernel, halo=halo),
        out_shape=(strips, strips, jax.ShapeDtypeStruct((2, c), F32)),
        in_specs=[vmem()] * len(args),
        out_specs=(vmem(),) * 3,
        scratch_shapes=[pltpu.VMEM((LINES * 16, c), F32)],
        compiler_params=params(4),
        name="cols",
    )(*args)


def over_axis(sums, axis):
    count = lax.axis_size(axis)
    return sums + sum(
        lax.ppermute(sums, axis, [(i, i ^ step) for i in range(count)]) for step in range(1, count)
    )


def everyone(sums):
    return over_axis(over_axis(sums, "ha"), "wa")


def exchange(head, tail, own, axis):
    return around(tail, axis, 1), around(head, axis, -1), around(own, axis, 2)


def over_axis(sums, axis):
    count = lax.axis_size(axis)
    return sums + sum(
        lax.ppermute(sums, axis, [(i, i ^ step) for i in range(count)]) for step in range(1, count)
    )


def everyone(sums):
    return over_axis(over_axis(sums, "ha"), "wa")


def local(frames, caches, conv_weights, conv_bias, norm_gain, norm_shift):
    n, rows, cols, c = frames.shape
    cells = float(n * rows * cols * lax.axis_size(("ha", "wa")) * (c // GROUPS))
    kept_n, convs = caches.shape[:2]
    weights = conv_weights.reshape(convs, 3, 9 * c, c)
    halo = Halo(rows, [(n, WIDTHS[0])] + [(kept_n, w) for w in WIDTHS])
    next_halo = Halo(rows, [(n, WIDTHS[2])])

    lines = jax.ShapeDtypeStruct((halo.count, cols, c), BF16)
    head, tail, own = pl.pallas_call(
        functools.partial(rows_kernel, halo=halo),
        out_shape=(lines, lines, jax.ShapeDtypeStruct((2, c), F32)),
        in_specs=[any_space()] * 2,
        out_specs=(vmem(),) * 3,
        scratch_shapes=[
            pltpu.VMEM(frames.shape, BF16),
            pltpu.SemaphoreType.DMA((n + 2 * (n + kept_n * convs),)),
        ],
        compiler_params=params(ROWS_MIB),
        name="rows",
    )(frames, caches)
    block, saved = frames, []
    for k in range(0, convs, 2):
        north, south, far = exchange(head, tail, own, "ha")
        head, tail, own = cols_part(
            next_halo if k else halo, block, () if k else (caches,), north, south, far, own
        )
        west, east, far = exchange(head, tail, own, "wa")
        if k == 0:
            sides = (north, south, west, east)
        field = (block, north, south, west, east, far, own)
        kept = kept_part(k, halo, caches, sides, weights, conv_bias)
        rest = (norm_gain, norm_shift, conv_bias, weights)
        middle, strips, sums, keep = main_part(
            k, halo, field, *rest, kept, (), None, None, cells
        )
        saved.append(keep)
        kept = kept_part(k + 1, halo, caches, sides, weights, conv_bias)
        field = (middle, strips, everyone(sums))
        last = k + 2 == convs
        done = main_part(
            k + 1,
            halo,
            field,
            *rest,
            kept,
            (block,),
            saved if last else None,
            next_halo.count,
            cells,
        )
        if last:
            return tuple(done)
        block, head, tail, own, keep = done
        saved.append(keep)


def solution(mesh):
    return jax.shard_map(
        local,
        mesh=mesh,
        in_specs=(
            P("clip", "ha", "wa", None),
            P("clip", None, "ha", "wa", None),
            P(),
            P(),
            P(),
            P(),
        ),
        out_specs=(P("clip", "ha", "wa", None), P("clip", None, "ha", "wa", None)),
        check_vma=False,
    )
```
